32 devices in a mesh: rep: 4 (over x, core), shard: 8 (over z, y).
Axes of the slice: x: 2, y: 2, z: 4, core: 2. Of those that a mesh axis runs over, the one named last changes fastest.
Arguments:
- latents: bfloat16 [2, 8, 1024, 1408], P(None, 'shard', 'rep'), may hold values from -6 to 6
- skip_branch: bfloat16 [2, 8, 1024, 1408], P(None, 'shard', 'rep'), may hold values from -6 to 6
- text_states: bfloat16 [2, 8, 256, 1024], P(None, 'shard'), may hold values from -6 to 6
- time_embed: bfloat16 [2, 8, 1408], P(None, 'shard'), may hold values from -6 to 6
- out_cotangent: bfloat16 [2, 8, 1024, 1408], P(None, 'shard', 'rep'), may hold values from -6 to 6
- skip_proj: bfloat16 [2816, 1408], P('shard'), may hold values from -0.109375 to 0.109375
- shift_proj: bfloat16 [1408, 1408], P('shard'), may hold values from -0.15625 to 0.15625
- self_proj_in: bfloat16 [1408, 4224], P('shard'), may hold values from -0.15625 to 0.15625
- self_proj_out: bfloat16 [1408, 1408], P('shard'), may hold values from -3 to 3
- cross_query: bfloat16 [1408, 1408], P('shard'), may hold values from -0.15625 to 0.15625
- cross_keyval: bfloat16 [1024, 2816], P('shard'), may hold values from -0.1875 to 0.1875
- cross_proj_out: bfloat16 [1408, 1408], P('shard'), may hold values from -1.5 to 1.5
- feed_up: bfloat16 [1408, 6144], P('shard'), may hold values from -0.15625 to 0.15625
- feed_down: bfloat16 [6144, 1408], P('shard'), may hold values from -0.078125 to 0.078125
- norm_gains: bfloat16 [5, 1408], P(None, 'shard'), may hold values from 0.5 to 1.5
- bias_rows: bfloat16 [16, 1408], P(None, 'shard'), may hold values from -1.1953125 to 1.1953125
- feed_up_bias: bfloat16 [6144], P('shard'), may hold values from -1.1953125 to 1.1953125
- head_gains: bfloat16 [4, 88], replicated, may hold values from 0.5 to 1.5
- head_biases: bfloat16 [3, 88], replicated, may hold values from -1.1953125 to 1.1953125
Outputs:
- activations: bfloat16 [2, 8, 1024, 1408], P(None, 'shard', 'rep')
- input_grad: float32 [2, 8, 1024, 1408], P(None, 'shard', 'rep')
- skip_grad: float32 [2, 8, 1024, 1408], P(None, 'shard', 'rep')
- text_grad: float32 [2, 8, 256, 1024], P(None, 'shard')
- skip_proj_grad: float32 [2816, 1408], P('shard')
- shift_proj_grad: float32 [1408, 1408], P('shard')
- self_in_grad: float32 [1408, 4224], P('shard')
- self_out_grad: float32 [1408, 1408], P('shard')
- cross_query_grad: float32 [1408, 1408], P('shard')
- cross_keyval_grad: float32 [1024, 2816], P('shard')
- cross_out_grad: float32 [1408, 1408], P('shard')
- feed_up_grad: float32 [1408, 6144], P('shard')
- feed_down_grad: float32 [6144, 1408], P('shard')
- norm_gains_grad: float32 [5, 1408], P(None, 'shard')
- bias_rows_grad: float32 [16, 1408], P(None, 'shard')
- feed_bias_grad: float32 [6144], P('shard')
- head_gains_grad: float32 [4, 88], replicated
- head_biases_grad: float32 [3, 88], replicated
The draws below stay inside these ranges and needn't reach their ends.
All inputs are finite; a program needn't handle non-finite values.
Results may differ from the reference program's by a relative error of at most 0.019.
Values may be sent and summed in bfloat16 or wider, within the bound.
A program may use at most 336 MiB of HBM per device.

```python
import jax
import jax.numpy as jnp
from jax import lax

D = 1408
FF = 6144
TEXT_D = 1024
TEXT = 256
GRID = 32
MB = 2
HD = 88
L = 1024
SEQS = 8


def level_of(own_key, dims, cuts, low, largest):
    level = 1.0
    for dim, shards_of in cuts:
        draws = jax.random.uniform(jax.random.fold_in(jax.random.fold_in(own_key, 6), dim), (shards_of,), jnp.float32, low / len(cuts), largest / len(cuts))
        level = level * jnp.repeat(jnp.exp(draws), dims[dim] // shards_of).reshape((-1,) + (1,) * (len(dims) - 1 - dim))
    return level


def bell_draw(own_key, dims, width, reach, pieces=(), kind=jnp.bfloat16):
    factor_of = level_of(own_key, dims, pieces, -0.22, 0.18) if pieces else 1.0
    result = jax.random.normal(own_key, dims, jnp.float32) * width * factor_of
    return jnp.minimum(jnp.maximum(result, -reach), reach).astype(kind)


def setup_inputs(seed: int = 0) -> dict:
    streams_of = jax.random.split(jax.random.key(seed), 20)
    latents = bell_draw(streams_of[0], (MB, SEQS, L, D), 1.0, 6.0, ((1, 8), (2, 4)))
    skip_branch = bell_draw(streams_of[1], (MB, SEQS, L, D), 1.0, 6.0, ((1, 8), (2, 4)))
    text_states = bell_draw(streams_of[2], (MB, SEQS, TEXT, TEXT_D), 1.0, 6.0, ((1, 8),))
    time_embed = bell_draw(streams_of[3], (MB, SEQS, D), 1.0, 6.0, ((1, 8),))
    out_cotangent = bell_draw(streams_of[4], (MB, SEQS, L, D), 1.0, 6.0, ((1, 8), (2, 4)))
    skip_proj = bell_draw(streams_of[5], (2 * D, D), (2 * D) ** -0.5, 0.109375, ((0, 8),))
    shift_proj = bell_draw(streams_of[6], (D, D), D ** -0.5, 0.15625, ((0, 8),))
    self_proj_in = bell_draw(streams_of[7], (D, 3 * D), D ** -0.5, 0.15625, ((0, 8),))
    self_proj_out = bell_draw(streams_of[8], (D, D), (max(1, D * 3 // L)) ** -0.5, 3.0, ((0, 8),))
    cross_query = bell_draw(streams_of[9], (D, D), D ** -0.5, 0.15625, ((0, 8),))
    cross_keyval = bell_draw(streams_of[10], (TEXT_D, 2 * D), TEXT_D ** -0.5, 0.1875, ((0, 8),))
    cross_proj_out = bell_draw(streams_of[11], (D, D), (max(1, D * 3 // TEXT)) ** -0.5, 1.5, ((0, 8),))
    feed_up = bell_draw(streams_of[12], (D, FF), D ** -0.5, 0.15625, ((0, 8),))
    feed_down = bell_draw(streams_of[13], (FF, D), FF ** -0.5, 0.078125, ((0, 8),))
    norm_gains = jnp.clip(1.0 + 0.1 * jax.random.normal(streams_of[14], (5, D), jnp.float32), 0.5, 1.5).astype(jnp.bfloat16)
    bias_rows = bell_draw(streams_of[15], (16, D), 0.2, 1.1953125, ((1, 8),))
    feed_up_bias = bell_draw(streams_of[16], (FF,), 0.2, 1.1953125, ((0, 8),))
    head_gains = jnp.clip(1.0 + 0.1 * jax.random.normal(streams_of[17], (4, HD), jnp.float32), 0.5, 1.5).astype(jnp.bfloat16)
    head_biases = bell_draw(streams_of[18], (3, HD), 0.2, 1.1953125)
    return {"latents": latents, "skip_branch": skip_branch, "text_states": text_states, "time_embed": time_embed, "out_cotangent": out_cotangent, "skip_proj": skip_proj, "shift_proj": shift_proj, "self_proj_in": self_proj_in, "self_proj_out": self_proj_out, "cross_query": cross_query, "cross_keyval": cross_keyval, "cross_proj_out": cross_proj_out, "feed_up": feed_up, "feed_down": feed_down, "norm_gains": norm_gains, "bias_rows": bias_rows, "feed_up_bias": feed_up_bias, "head_gains": head_gains, "head_biases": head_biases}


@jax.custom_vjp
def low(v):
    return lax.optimization_barrier(v.astype(jnp.bfloat16)).astype(jnp.float32)

@jax.custom_vjp
def low_back(v):
    return v

def low_keep(v):
    return (low(v), None)

def low_pass(kept, grad):
    return (grad,)

def back_keep(v):
    return (v, None)

def back_low(kept, grad):
    return (low(grad),)
low.defvjp(low_keep, low_pass)
low_back.defvjp(back_keep, back_low)
highest = lax.Precision.HIGHEST

def layer_norm(operand, scales, offsets):
    row_mean = lax.optimization_barrier(jnp.mean(operand, -1, keepdims=True))
    centred = operand - row_mean
    spread = lax.optimization_barrier(jnp.mean(centred * centred, -1, keepdims=True))
    return centred * lax.rsqrt(spread + 1e-06) * scales + offsets

def dense(operand, weight, offsets):
    return low_back(jnp.dot(low(operand), weight, precision=highest)) + offsets

def rotary_tables(positions):
    pair_index = jnp.arange(HD // 4, dtype=jnp.float32)
    frequency = 10000.0 ** (-2.0 * pair_index / (HD // 2))
    row_coord = (positions // GRID).astype(jnp.float32)
    column_coord = (positions % GRID).astype(jnp.float32)
    angles = jnp.concatenate([row_coord[:, None] * frequency[None, :], column_coord[:, None] * frequency[None, :]], axis=1)
    return (jnp.cos(angles), jnp.sin(angles))

def rotate(heads_in, cosine_table, sine_table):
    paired = heads_in.reshape(heads_in.shape[0], heads_in.shape[1], HD // 2, 2)
    even_part = paired[..., 0]
    odd_part = paired[..., 1]
    cosine_rows = cosine_table[:, None, :]
    sine_rows = sine_table[:, None, :]
    turned = jnp.stack([even_part * cosine_rows - odd_part * sine_rows, even_part * sine_rows + odd_part * cosine_rows], axis=-1)
    return turned.reshape(heads_in.shape)

def head_view(matrix):
    return matrix.reshape(matrix.shape[0], -1, HD)

def attend(queries, keys_all, values_all):
    scores = jnp.einsum('qhd,khd->hqk', low(queries), low(keys_all), precision=highest) * HD ** (-0.5)
    soft_weights = jax.nn.softmax(low_back(scores), axis=-1)
    mixed_out = jnp.einsum('hqk,khd->qhd', low(soft_weights), low(values_all), precision=highest)
    return low_back(mixed_out)

def block(latent_seq, skip_seq, text_seq, time_seq, params):
    skip_proj, shift_proj, self_proj_in, self_proj_out, cross_query, cross_keyval, cross_proj_out, feed_up, feed_down, norm_gains, bias_rows, feed_up_bias, head_gains, head_biases = params
    tok_count = latent_seq.shape[0]
    joined = jnp.concatenate([latent_seq, skip_seq], axis=1)
    normed = layer_norm(joined, jnp.concatenate([norm_gains[0], norm_gains[1]]), jnp.concatenate([bias_rows[0], bias_rows[1]]))
    hidden = dense(normed, skip_proj, bias_rows[2])
    shift_vec = jnp.dot(low(jax.nn.silu(time_seq)), shift_proj, precision=highest) + bias_rows[4]
    first_norm = layer_norm(hidden, norm_gains[2], bias_rows[3]) + shift_vec
    projected = dense(first_norm, self_proj_in, bias_rows[5:8].reshape(-1))
    cosine_table, sine_table = rotary_tables(jnp.arange(tok_count, dtype=jnp.int32))
    queries = rotate(layer_norm(head_view(projected[:, :D]), head_gains[0], head_biases[0]), cosine_table, sine_table)
    keys_all = rotate(layer_norm(head_view(projected[:, D:2 * D]), head_gains[1], head_biases[1]), cosine_table, sine_table)
    values_all = head_view(projected[:, 2 * D:])
    self_mixed = attend(queries, keys_all, values_all).reshape(tok_count, D)
    hidden = hidden + dense(self_mixed, self_proj_out, bias_rows[8])
    second = layer_norm(hidden, norm_gains[3], bias_rows[9])
    cross_queries = layer_norm(head_view(dense(second, cross_query, bias_rows[10])), head_gains[2], head_biases[2])
    text_keyval = dense(text_seq, cross_keyval, bias_rows[11:13].reshape(-1))
    text_keys = layer_norm(head_view(text_keyval[:, :D]), head_gains[3], 0.0)
    text_values = head_view(text_keyval[:, D:])
    cross_mixed = attend(cross_queries, text_keys, text_values).reshape(tok_count, D)
    hidden = hidden + dense(cross_mixed, cross_proj_out, bias_rows[13])
    third_norm = layer_norm(hidden, norm_gains[4], bias_rows[14])
    gelu_out = jax.nn.gelu(dense(third_norm, feed_up, feed_up_bias), approximate=True)
    return hidden + dense(gelu_out, feed_down, bias_rows[15])

def reference(latents, skip_branch, text_states, time_embed, out_cotangent, skip_proj, shift_proj, self_proj_in, self_proj_out, cross_query, cross_keyval, cross_proj_out, feed_up, feed_down, norm_gains, bias_rows, feed_up_bias, head_gains, head_biases):
    params = tuple((tensor.astype(jnp.float32) for tensor in (skip_proj, shift_proj, self_proj_in, self_proj_out, cross_query, cross_keyval, cross_proj_out, feed_up, feed_down, norm_gains, bias_rows, feed_up_bias, head_gains, head_biases)))
    seq_total = MB * SEQS
    latent_all = latents.astype(jnp.float32).reshape(seq_total, L, D)
    skip_all = skip_branch.astype(jnp.float32).reshape(seq_total, L, D)
    text_all = text_states.astype(jnp.float32).reshape(seq_total, TEXT, TEXT_D)
    time_all = time_embed.astype(jnp.float32).reshape(seq_total, D)

    def forward(latent_in, skip_in, text_in, weights_in):

        def one_seq(members):
            return block(members[0], members[1], members[2], members[3], weights_in)
        stored = jax.checkpoint(one_seq)
        return lax.map(stored, (latent_in, skip_in, text_in, time_all))
    outputs, pullback = jax.vjp(forward, latent_all, skip_all, text_all, params)
    gradients = pullback(out_cotangent.astype(jnp.float32).reshape(seq_total, L, D))
    weight_grads = gradients[3]
    return (outputs.reshape(MB, SEQS, L, D).astype(jnp.bfloat16), gradients[0].reshape(MB, SEQS, L, D), gradients[1].reshape(MB, SEQS, L, D), gradients[2].reshape(MB, SEQS, TEXT, TEXT_D), weight_grads[0], weight_grads[1], weight_grads[2], weight_grads[3], weight_grads[4], weight_grads[5], weight_grads[6], weight_grads[7], weight_grads[8], weight_grads[9], weight_grads[10], weight_grads[11], weight_grads[12], weight_grads[13])
```

```python
from functools import partial

import jax
import jax.numpy as jnp
import numpy as np
from jax import lax
from jax.experimental import pallas as pl
from jax.experimental.pallas import tpu as pltpu
from jax.sharding import PartitionSpec as P

D = 1408
GRID = 32
MB = 2
HD = 88


def layer_norm(operand, scales, offsets):
    row_mean = jnp.mean(operand, -1, keepdims=True)
    centred = operand - row_mean
    spread = jnp.mean(centred * centred, -1, keepdims=True)
    return centred * lax.rsqrt(spread + 1e-06) * scales + offsets


def rotary_tables(positions):
    pair_index = jnp.arange(HD // 4, dtype=jnp.float32)
    frequency = 10000.0 ** (-2.0 * pair_index / (HD // 2))
    row_coord = (positions // GRID).astype(jnp.float32)
    column_coord = (positions % GRID).astype(jnp.float32)
    angles = jnp.concatenate(
        [row_coord[:, None] * frequency[None, :], column_coord[:, None] * frequency[None, :]],
        axis=1,
    )
    return (jnp.cos(angles), jnp.sin(angles))


def rotate(heads_in, cosine_table, sine_table):
    paired = heads_in.reshape(heads_in.shape[0], heads_in.shape[1], HD // 2, 2)
    even_part = paired[..., 0]
    odd_part = paired[..., 1]
    cosine_rows = cosine_table[:, None, :]
    sine_rows = sine_table[:, None, :]
    turned = jnp.stack(
        [
            even_part * cosine_rows - odd_part * sine_rows,
            even_part * sine_rows + odd_part * cosine_rows,
        ],
        axis=-1,
    )
    return turned.reshape(heads_in.shape)


def head_view(matrix):
    return matrix.reshape(matrix.shape[0], -1, HD)


def product(left_side, right_side):
    return jnp.dot(left_side, right_side, preferred_element_type=jnp.float32)


def weight_grad(left_side, right_side):
    return lax.dot_general(
        left_side, right_side, (((0,), (0,)), ((), ())), preferred_element_type=jnp.float32
    )


def back_product(grad_rows, weight):
    return lax.dot_general(
        grad_rows, weight, (((1,), (1,)), ((), ())), preferred_element_type=jnp.float32
    )


def attend_forward(queries, keys_all, values_all):
    head_count = queries.shape[1]
    per_group = head_count // 4
    score_scale = HD ** (-0.5)

    def one_group(head_start):
        query_part = lax.dynamic_slice_in_dim(queries, head_start, per_group, 1)
        key_part = lax.dynamic_slice_in_dim(keys_all, head_start, per_group, 1)
        value_part = lax.dynamic_slice_in_dim(values_all, head_start, per_group, 1)
        scores = (
            jnp.einsum("qhd,khd->hqk", query_part, key_part, preferred_element_type=jnp.float32)
            * score_scale
        )
        row_max = jnp.max(scores, -1, keepdims=True)
        exponent = jnp.exp(scores - row_max)
        row_sum = jnp.sum(exponent, -1, keepdims=True)
        soft_weights = (exponent / row_sum).astype(jnp.bfloat16)
        mixed_out = jnp.einsum(
            "hqk,khd->qhd", soft_weights, value_part, preferred_element_type=jnp.float32
        )
        return (mixed_out, (row_max + jnp.log(row_sum))[..., 0])

    starts = jnp.arange(4, dtype=jnp.int32) * per_group
    mixed_out, log_total = lax.map(one_group, starts)
    tok_count = queries.shape[0]
    mixed_out = jnp.moveaxis(mixed_out, 0, 1).reshape(tok_count, head_count * HD)
    return (mixed_out, log_total.reshape(head_count, tok_count))


def attend_backward(queries, keys_all, values_all, log_total, grad_mixed):
    head_count = queries.shape[1]
    per_group = head_count // 4
    score_scale = HD ** (-0.5)

    def one_group(head_start):
        query_part = lax.dynamic_slice_in_dim(queries, head_start, per_group, 1)
        key_part = lax.dynamic_slice_in_dim(keys_all, head_start, per_group, 1)
        value_part = lax.dynamic_slice_in_dim(values_all, head_start, per_group, 1)
        grad_part = lax.dynamic_slice_in_dim(grad_mixed, head_start, per_group, 1)
        log_part = lax.dynamic_slice_in_dim(log_total, head_start, per_group, 0)
        scores = (
            jnp.einsum("qhd,khd->hqk", query_part, key_part, preferred_element_type=jnp.float32)
            * score_scale
        )
        soft_weights = jnp.exp(scores - log_part[..., None])
        grad_weights = jnp.einsum(
            "qhd,khd->hqk", grad_part, value_part, preferred_element_type=jnp.float32
        )
        row_inner = jnp.sum(soft_weights * grad_weights, -1, keepdims=True)
        grad_scores = (soft_weights * (grad_weights - row_inner)).astype(jnp.bfloat16)
        grad_query = (
            jnp.einsum("hqk,khd->qhd", grad_scores, key_part, preferred_element_type=jnp.float32)
            * score_scale
        )
        grad_key = (
            jnp.einsum("hqk,qhd->khd", grad_scores, query_part, preferred_element_type=jnp.float32)
            * score_scale
        )
        grad_value = jnp.einsum(
            "hqk,qhd->khd",
            soft_weights.astype(jnp.bfloat16),
            grad_part,
            preferred_element_type=jnp.float32,
        )
        return (grad_query, grad_key, grad_value)

    starts = jnp.arange(4, dtype=jnp.int32) * per_group
    grad_query, grad_key, grad_value = lax.map(one_group, starts)
    grad_query = jnp.moveaxis(grad_query, 0, 1).reshape(queries.shape[0], head_count, HD)
    grad_key = jnp.moveaxis(grad_key, 0, 1).reshape(keys_all.shape[0], head_count, HD)
    grad_value = jnp.moveaxis(grad_value, 0, 1).reshape(keys_all.shape[0], head_count, HD)
    return (grad_query, grad_key, grad_value)


def uninitialised(shape, dtype):
    return pl.pallas_call(
        lambda out_ref: None,
        out_shape=jax.ShapeDtypeStruct(shape, dtype),
        out_specs=pl.BlockSpec(memory_space=pl.ANY),
        compiler_params=pltpu.CompilerParams(has_side_effects=True),
    )()


class Links:
    def __init__(self, shard_count, rep_count):
        self.n = shard_count
        self.reps = rep_count
        self.ring = shard_count == 8 and rep_count == 4
        self.half = shard_count // 2
        order = list(range(0, shard_count, 2)) + list(range(shard_count - 1, 0, -2))
        self.order = np.asarray(order, np.int32)
        self.shard = lax.axis_index("shard")
        rep = lax.axis_index("rep")
        self.core = rep % 2
        self.side = rep // 2
        self.sign = 1 - 2 * self.core
        self.position = jnp.asarray(np.argsort(order).astype(np.int32))[self.shard]
        perm = []
        for r in range(rep_count):
            for q in range(shard_count):
                step = 1 if r % 2 == 0 else -1
                perm.append(
                    (
                        r * shard_count + order[q],
                        r * shard_count + order[(q + step) % shard_count],
                    )
                )
        self.ring_perm = perm
        self.core_perm = [(r, r ^ 1) for r in range(rep_count)]
        self.side_perm = [(r, r ^ 2) for r in range(rep_count)]
        self.sent = []

    def at(self, distance):
        return jnp.asarray(self.order)[(self.position + distance + 2 * self.n) % self.n]

    def along_ring(self, block, depth=2):
        if len(self.sent) >= depth:
            block, _ = lax.optimization_barrier((block, self.sent[-depth]))
        moved = lax.ppermute(block, ("rep", "shard"), self.ring_perm)
        self.sent.append(moved)
        return moved

    def swap_core(self, block):
        return lax.ppermute(block, "rep", self.core_perm)

    def swap_side(self, block):
        return lax.ppermute(block, "rep", self.side_perm)


def pick(stack, index):
    return lax.dynamic_index_in_dim(stack, index, 0, keepdims=False)


def place(stack, block, index, row=0):
    return lax.dynamic_update_slice(stack, block[None], (index, row, 0))


def gather_steps(links, piece):
    arrived = []
    block = piece
    for _ in range(1, links.half):
        block = yield block
        arrived.append(block)
    rows = piece.shape[0] // 2
    last = lax.dynamic_slice_in_dim(block, links.core * rows, rows, 0)
    arrived.append((yield last))
    return arrived


def run_steps(links, generators, sequence):
    waiting = {name: next(gen) for name, gen in generators.items()}
    results = {}
    for name in sequence:
        moved = links.along_ring(waiting[name])
        try:
            waiting[name] = generators[name].send(moved)
        except StopIteration as stop:
            results[name] = stop.value
    return results


def lots(arrived):
    return [jnp.concatenate(arrived[:2], 0), jnp.concatenate(arrived[2:], 0)]


def unlots(pair, rows):
    first, second = pair
    return [first[:rows], first[rows:], second[:rows], second[rows:]]


def store_arrivals(links, stack, own, mine, other, row_range):
    low, high = row_range
    total = own.shape[0]
    rows = total // 2
    width = high - low
    stack = place(stack, own[low:high], links.shard)
    for k in range(1, links.half):
        stack = place(stack, mine[k - 1][low:high], links.at(-links.sign * k))
        stack = place(stack, other[k - 1][low:high], links.at(links.sign * k))
    far = links.at(links.half)
    both = jnp.where(
        links.core == 0,
        jnp.concatenate([mine[-1], other[-1]], 0),
        jnp.concatenate([other[-1], mine[-1]], 0),
    )
    stack = place(stack, both[low:high], far)
    return stack


def gather_finish(links, own, arrived, parts):
    rows = own.shape[0]
    other = unlots([links.swap_core(lot) for lot in lots(arrived)], rows)
    wholes = []
    for low, high in parts:
        stack = uninitialised((links.n, high - low, own.shape[1]), own.dtype)
        wholes.append(store_arrivals(links, stack, own, arrived, other, (low, high)))
    return wholes


def gather_finish_halved(links, own, far_own, arrived):
    rows = own.shape[0]
    whole = (0, rows)
    pair = lots(arrived)
    far_pair = [links.swap_side(lot) for lot in pair]
    other, far_other = [], []
    for near_lot, far_lot in zip(pair, far_pair):
        moved = links.swap_core(jnp.concatenate([near_lot, far_lot], 0))
        other.append(moved[: near_lot.shape[0]])
        far_other.append(moved[near_lot.shape[0] :])
    shape = (links.n, rows, own.shape[1])
    near = store_arrivals(
        links, uninitialised(shape, own.dtype), own, arrived, unlots(other, rows), whole
    )
    far = store_arrivals(
        links,
        uninitialised(shape, own.dtype),
        far_own,
        unlots(far_pair, rows),
        unlots(far_other, rows),
        whole,
    )
    return near, far


def total32(*terms):
    total = terms[0].astype(jnp.float32)
    for term in terms[1:]:
        total = total + term.astype(jnp.float32)
    return total


def handled(links, stack, sign):
    blocks = [pick(stack, links.at(sign * k)) for k in range(1, links.half)]
    rows = stack.shape[1] // 2
    core = jnp.where(sign == links.sign, links.core, 1 - links.core)
    blocks.append(lax.dynamic_slice_in_dim(pick(stack, links.at(links.half)), core * rows, rows, 0))
    return blocks


def reduce_ring(links, blocks):
    rows = blocks[-1].shape[0]
    moved = yield blocks[-1]
    top = jnp.zeros_like(moved)
    full = jnp.where(
        links.core == 0,
        jnp.concatenate([moved, top], 0),
        jnp.concatenate([top, moved], 0),
    )
    for k in range(links.half - 1, 0, -1):
        full = yield total32(blocks[k - 1], full).astype(jnp.bfloat16)
    return full


def reduce_start(links, stack):
    rows = stack.shape[1]
    out = jnp.concatenate(handled(links, stack, -links.sign), 0)
    got = links.swap_core(out)
    mine = handled(links, stack, links.sign)
    blocks = []
    for k, block in enumerate(mine):
        part = got[k * rows : k * rows + block.shape[0]]
        blocks.append(total32(block, part).astype(jnp.bfloat16))
    return blocks


def reduce_finish(links, stack, moved):
    rows = stack.shape[1]
    mine = total32(pick(stack, links.shard), moved).astype(jnp.bfloat16)
    chip = total32(mine, links.swap_core(mine)).astype(jnp.bfloat16)
    half = lax.dynamic_slice_in_dim(chip, links.core * (rows // 2), rows // 2, 0)
    half = total32(half, links.swap_side(half)).astype(jnp.bfloat16)
    other = links.swap_core(half)
    return jnp.where(
        links.core == 0,
        jnp.concatenate([half, other], 0),
        jnp.concatenate([other, half], 0),
    ).astype(jnp.float32)


def reduce_start_halved(links, near, far):
    rows = near.shape[1]
    near_blocks = reduce_start_list(links, [near, far])
    mine, theirs = near_blocks
    out = jnp.concatenate(theirs + [pick(far, links.shard)], 0)
    got = links.swap_side(out)
    blocks = []
    for k, block in enumerate(mine):
        part = got[k * rows : k * rows + block.shape[0]]
        blocks.append(total32(block, part).astype(jnp.bfloat16))
    return blocks, got[-rows:]


def reduce_start_list(links, stacks):
    rows = stacks[0].shape[1]
    sends = [jnp.concatenate(handled(links, stack, -links.sign), 0) for stack in stacks]
    got = links.swap_core(jnp.concatenate(sends, 0))
    results = []
    for j, stack in enumerate(stacks):
        base = j * sends[0].shape[0]
        blocks = []
        for k, block in enumerate(handled(links, stack, links.sign)):
            part = got[base + k * rows : base + k * rows + block.shape[0]]
            blocks.append(total32(block, part).astype(jnp.bfloat16))
        results.append(blocks)
    return results


def reduce_finish_halved(links, near, own_far, moved):
    mine = total32(pick(near, links.shard), own_far, moved).astype(jnp.bfloat16)
    total = total32(mine, links.swap_core(mine)).astype(jnp.bfloat16)
    other = links.swap_side(total)
    first = jnp.where(links.side == 0, total, other).astype(jnp.float32)
    second = jnp.where(links.side == 0, other, total).astype(jnp.float32)
    return first, second


def shards(
    shard_count,
    rep_count,
    latents,
    skip_branch,
    text_states,
    time_embed,
    out_cotangent,
    skip_proj,
    shift_proj,
    self_proj_in,
    self_proj_out,
    cross_query,
    cross_keyval,
    cross_proj_out,
    feed_up,
    feed_down,
    norm_gains,
    bias_rows,
    feed_up_bias,
    head_gains,
    head_biases,
):
    links = Links(shard_count, rep_count)
    n = shard_count
    batches, _, local_tokens, _ = latents.shape
    rows_all = batches * local_tokens
    hidden_units = feed_up.shape[1]
    slab = feed_down.shape[0] // 2
    own_rows = shift_proj.shape[0]
    text_depth = cross_keyval.shape[0]
    positions = lax.axis_index("rep") * local_tokens + jnp.arange(local_tokens, dtype=jnp.int32)
    positions = jnp.tile(positions, batches)
    cosine_table, sine_table = rotary_tables(positions)
    head_scales = head_gains.astype(jnp.float32)
    head_shifts = head_biases.astype(jnp.float32)

    def self_heads(query_raw, key_raw, gain_query, bias_query, gain_key, bias_key):
        return (
            rotate(
                layer_norm(head_view(query_raw), gain_query, bias_query), cosine_table, sine_table
            ),
            rotate(layer_norm(head_view(key_raw), gain_key, bias_key), cosine_table, sine_table),
        )

    def cross_heads(query_raw, key_raw, gain_query, bias_query, gain_key):
        return (
            layer_norm(head_view(query_raw), gain_query, bias_query),
            layer_norm(head_view(key_raw), gain_key, 0.0),
        )

    silu_own = jax.nn.silu(time_embed[:, 0].astype(jnp.float32)).astype(jnp.bfloat16)
    flat = jnp.concatenate(
        [norm_gains.reshape(-1), bias_rows.reshape(-1), feed_up_bias, silu_own.reshape(-1)]
    )
    vectors = lax.all_gather(flat[None], "shard", axis=0, tiled=True)
    cut_a = norm_gains.size
    cut_b = cut_a + bias_rows.size
    cut_c = cut_b + feed_up_bias.size
    gain_rows = jnp.moveaxis(vectors[:, :cut_a].reshape(n, norm_gains.shape[0], -1), 0, 1)
    gain_rows = gain_rows.reshape(norm_gains.shape[0], D).astype(jnp.float32)
    bias_vals = jnp.moveaxis(vectors[:, cut_a:cut_b].reshape(n, bias_rows.shape[0], -1), 0, 1)
    bias_vals = bias_vals.reshape(bias_rows.shape[0], D).astype(jnp.float32)
    up_offsets = vectors[:, cut_b:cut_c].astype(jnp.float32).reshape(n, 2, slab)
    silu_all = vectors[:, cut_c:].reshape(n * batches, D)

    silu_cols = lax.dynamic_slice_in_dim(silu_all, links.shard * own_rows, own_rows, 1)
    shift_terms = product(silu_cols, shift_proj).reshape(n, batches, D)
    shift_own = lax.psum_scatter(shift_terms, "shard", scatter_dimension=0, tiled=True)[0]
    shift_vec = shift_own + bias_vals[4]

    up_split = feed_up.reshape(own_rows, n, 2, slab)
    up_near = lax.dynamic_index_in_dim(up_split, links.side, 2, keepdims=False).reshape(own_rows, -1)
    up_far = lax.dynamic_index_in_dim(up_split, 1 - links.side, 2, keepdims=False)
    up_far = up_far.reshape(own_rows, -1)
    down_near = lax.dynamic_slice_in_dim(feed_down, links.side * slab, slab, 0)
    down_far = lax.dynamic_slice_in_dim(feed_down, (1 - links.side) * slab, slab, 0)
    keyval_rows = jnp.concatenate([cross_keyval[:, :D], cross_keyval[:, D:]], 0)
    small = jnp.concatenate([self_proj_out, cross_query, cross_proj_out, keyval_rows], 0)
    cuts = [0, own_rows, 2 * own_rows, 3 * own_rows, 3 * own_rows + text_depth]
    cuts.append(cuts[-1] + text_depth)
    small_parts = list(zip(cuts[:-1], cuts[1:]))
    if links.ring:
        arrivals = run_steps(
            links,
            {
                "skip": gather_steps(links, skip_proj),
                "in": gather_steps(links, self_proj_in),
                "small": gather_steps(links, small),
                "up": gather_steps(links, up_near),
                "down": gather_steps(links, down_near),
            },
            ["skip", "in"] * 4
            + ["up", "small", "up", "small", "up", "small", "up", "down"]
            + ["small", "down", "down", "down"],
        )
        (skip_stack,) = gather_finish(links, skip_proj, arrivals["skip"], [(0, skip_proj.shape[0])])
        (in_stack,) = gather_finish(links, self_proj_in, arrivals["in"], [(0, own_rows)])
        small_stacks = gather_finish(links, small, arrivals["small"], small_parts)
        up_stacks = gather_finish_halved(links, up_near, up_far, arrivals["up"])
        down_stacks = gather_finish_halved(links, down_near, down_far, arrivals["down"])
    else:

        def whole(block):
            return lax.all_gather(block, "shard", axis=0)

        skip_stack, in_stack = whole(skip_proj), whole(self_proj_in)
        small_stacks = [whole(small[low:high]) for low, high in small_parts]
        up_stacks = (whole(up_near), whole(up_far))
        down_stacks = (whole(down_near), whole(down_far))
    skip_full = skip_stack.reshape(-1, D)
    proj_in_full = in_stack.reshape(D, -1)
    proj_out_full = small_stacks[0].reshape(D, D)
    query_full = small_stacks[1].reshape(D, D)
    cross_out_full = small_stacks[2].reshape(D, D)
    text_key_full = small_stacks[3].reshape(-1, D)
    text_value_full = small_stacks[4].reshape(-1, D)
    up_halves = [stack.reshape(D, -1) for stack in up_stacks]
    down_halves = [stack.reshape(-1, D) for stack in down_stacks]
    up_bias_halves = [
        lax.dynamic_index_in_dim(up_offsets, side, 1, keepdims=False).reshape(-1)
        for side in (links.side, 1 - links.side)
    ]

    latent_rows = latents.reshape(rows_all, D).astype(jnp.float32)
    skip_rows = skip_branch.reshape(rows_all, D).astype(jnp.float32)
    text_rows = text_states.reshape(-1, text_states.shape[-1])
    joined = jnp.concatenate([latent_rows, skip_rows], axis=1)
    gain_cat = jnp.concatenate([gain_rows[0], gain_rows[1]])
    bias_cat = jnp.concatenate([bias_vals[0], bias_vals[1]])
    normed, joined_pull = jax.vjp(layer_norm, joined, gain_cat, bias_cat)
    normed_low = normed.astype(jnp.bfloat16)
    hidden = product(normed_low, skip_full) + bias_vals[2]
    first_ln, first_pull = jax.vjp(layer_norm, hidden, gain_rows[2], bias_vals[3])
    first_low = (first_ln.reshape(batches, local_tokens, D) + shift_vec[:, None]).reshape(
        rows_all, D
    )
    first_low = first_low.astype(jnp.bfloat16)
    projected = product(first_low, proj_in_full) + bias_vals[5:8].reshape(-1)
    query_raw = projected[:, :D]
    key_raw = projected[:, D : 2 * D]
    value_raw = projected[:, 2 * D :]
    (query_rot, key_rot), self_pull = jax.vjp(
        self_heads,
        query_raw,
        key_raw,
        head_scales[0],
        head_shifts[0],
        head_scales[1],
        head_shifts[1],
    )
    query_low = query_rot.astype(jnp.bfloat16)
    key_low = key_rot.reshape(rows_all, D).astype(jnp.bfloat16)
    value_low = value_raw.astype(jnp.bfloat16)
    keyval_own = jnp.stack([key_low, value_low])
    if links.ring:
        keyval_side = links.swap_side(keyval_own)
        keyval_core = links.swap_core(keyval_own)
        keyval_both = links.swap_core(keyval_side)
        slots = jnp.stack([keyval_own, keyval_core, keyval_side, keyval_both])
    else:
        slots = lax.all_gather(keyval_own, "rep", axis=0)
    slots = slots.reshape(rep_count, 2, batches, local_tokens, D)

    def batch_of(tensor, index):
        step = tensor.shape[0] // batches
        return tensor[index * step : (index + 1) * step]

    self_saved = []
    self_parts = []
    for b in range(batches):
        keys_seq = head_view(slots[:, 0, b].reshape(-1, D))
        values_seq = head_view(slots[:, 1, b].reshape(-1, D))
        query_part = batch_of(query_low, b)
        mixed, log_total = attend_forward(query_part, keys_seq, values_seq)
        self_saved.append((query_part, keys_seq, values_seq, log_total))
        self_parts.append(mixed.astype(jnp.bfloat16))
    self_low = jnp.concatenate(self_parts, 0)
    hidden_two = hidden + product(self_low, proj_out_full) + bias_vals[8]
    second, second_pull = jax.vjp(layer_norm, hidden_two, gain_rows[3], bias_vals[9])
    second_low = second.astype(jnp.bfloat16)
    query_cross_raw = product(second_low, query_full) + bias_vals[10]
    text_key_raw = product(text_rows, text_key_full) + bias_vals[11]
    text_value_raw = product(text_rows, text_value_full) + bias_vals[12]
    (cross_queries, text_keys), cross_pull = jax.vjp(
        cross_heads,
        query_cross_raw,
        text_key_raw,
        head_scales[2],
        head_shifts[2],
        head_scales[3],
    )
    cross_low = cross_queries.astype(jnp.bfloat16)
    text_key_low = text_keys.astype(jnp.bfloat16)
    text_value_low = head_view(text_value_raw).astype(jnp.bfloat16)
    cross_saved = []
    cross_parts = []
    for b in range(batches):
        part = (batch_of(cross_low, b), batch_of(text_key_low, b), batch_of(text_value_low, b))
        mixed, log_total = attend_forward(*part)
        cross_saved.append(part + (log_total,))
        cross_parts.append(mixed.astype(jnp.bfloat16))
    cross_out_low = jnp.concatenate(cross_parts, 0)
    hidden_three = hidden_two + product(cross_out_low, cross_out_full) + bias_vals[13]
    third_norm, third_pull = jax.vjp(layer_norm, hidden_three, gain_rows[4], bias_vals[14])
    third_low = third_norm.astype(jnp.bfloat16)
    result = hidden_three + bias_vals[15]
    gelu_lows, gelu_pulls = [], []
    for up_half, down_half, up_bias in zip(up_halves, down_halves, up_bias_halves):
        up_out = product(third_low, up_half) + up_bias
        gelu_val, gelu_pull = jax.vjp(partial(jax.nn.gelu, approximate=True), up_out)
        gelu_lows.append(gelu_val.astype(jnp.bfloat16))
        gelu_pulls.append(gelu_pull)
        result = result + product(gelu_lows[-1], down_half)
    activations = result.astype(jnp.bfloat16).reshape(latents.shape)

    def term(left_side, right_side):
        grads = weight_grad(left_side, right_side).astype(jnp.bfloat16)
        return grads.reshape(n, -1, grads.shape[-1])

    grad_low = out_cotangent.reshape(rows_all, D)
    grad_out = grad_low.astype(jnp.float32)
    grad_up_lows, grad_up_sums = [], []
    grad_third = None
    for up_half, down_half, gelu_pull in zip(up_halves, down_halves, gelu_pulls):
        grad_up = gelu_pull(back_product(grad_low, down_half))[0]
        grad_up_sums.append(jnp.sum(grad_up, 0))
        grad_up_lows.append(grad_up.astype(jnp.bfloat16))
        share = back_product(grad_up_lows[-1], up_half)
        grad_third = share if grad_third is None else grad_third + share
    down_terms = [term(gelu_low, grad_low) for gelu_low in gelu_lows]
    up_terms = [term(third_low, part) for part in grad_up_lows]
    three_part, gain_last, bias_last = third_pull(grad_third)
    grad_three = grad_out + three_part
    grad_three_low = grad_three.astype(jnp.bfloat16)
    cross_out_term = term(cross_out_low, grad_three_low)
    grad_cross_mixed = back_product(grad_three_low, cross_out_full).astype(jnp.bfloat16)
    pieces = [
        attend_backward(*cross_saved[b], head_view(batch_of(grad_cross_mixed, b)))
        for b in range(batches)
    ]
    grad_cq, grad_tk, grad_tv = (jnp.concatenate(list(part), 0) for part in zip(*pieces))
    grad_cq_raw, grad_tk_raw, cross_gain_grad, cross_bias_grad, text_gain_grad = cross_pull(
        (grad_cq, grad_tk)
    )
    grad_cq_low = grad_cq_raw.astype(jnp.bfloat16)
    query_term = term(second_low, grad_cq_low)
    grad_second = back_product(grad_cq_low, query_full)
    grad_tv_raw = grad_tv.reshape(grad_tv.shape[0], D)
    grad_tk_low = grad_tk_raw.astype(jnp.bfloat16)
    grad_tv_low = grad_tv_raw.astype(jnp.bfloat16)
    text_key_term = term(text_rows, grad_tk_low)
    text_value_term = term(text_rows, grad_tv_low)
    text_grad = back_product(grad_tk_low, text_key_full) + back_product(
        grad_tv_low, text_value_full
    )
    text_grad = lax.psum(text_grad.astype(jnp.bfloat16), "rep").astype(jnp.float32)
    two_part, gain_mid, bias_mid = second_pull(grad_second)
    grad_two = grad_three + two_part
    grad_two_low = grad_two.astype(jnp.bfloat16)
    proj_out_term = term(self_low, grad_two_low)
    small_term = jnp.concatenate(
        [proj_out_term, query_term, cross_out_term, text_key_term, text_value_term], 1
    )
    grad_self_mixed = back_product(grad_two_low, proj_out_full).astype(jnp.bfloat16)
    pieces = [
        attend_backward(*self_saved[b], head_view(batch_of(grad_self_mixed, b)))
        for b in range(batches)
    ]
    grad_query = jnp.concatenate([part[0] for part in pieces], 0)
    grad_slots = jnp.stack(
        [
            jnp.stack([part[j].reshape(rep_count, local_tokens, D) for part in pieces], 1)
            for j in (1, 2)
        ],
        1,
    ).astype(jnp.bfloat16)
    if links.ring:
        got = links.swap_core(jnp.stack([grad_slots[1], grad_slots[3]]))
        chip = total32(jnp.stack([grad_slots[0], grad_slots[2]]), got)
        got = links.swap_side(chip[1].astype(jnp.bfloat16))
        grad_keyval_own = total32(chip[0], got)
    else:
        grad_keyval_own = lax.psum_scatter(
            grad_slots, "rep", scatter_dimension=0, tiled=True
        )[0].astype(jnp.float32)
    grad_key_rows = grad_keyval_own[0].reshape(rows_all, D)
    grad_value_rows = grad_keyval_own[1].reshape(rows_all, D)
    (
        grad_q_raw,
        grad_k_raw,
        self_qgain_grad,
        self_qbias_grad,
        self_kgain_grad,
        self_kbias_grad,
    ) = self_pull((grad_query, head_view(grad_key_rows)))
    grad_proj = jnp.concatenate([grad_q_raw, grad_k_raw, grad_value_rows], axis=1)
    grad_proj_low = grad_proj.astype(jnp.bfloat16)
    in_term = term(first_low, grad_proj_low)
    grad_first = back_product(grad_proj_low, proj_in_full)
    shift_grads = jnp.sum(grad_first.reshape(batches, local_tokens, D), 1)
    one_part, gain_first, bias_first = first_pull(grad_first)
    grad_hidden = grad_two + one_part
    grad_hidden_low = grad_hidden.astype(jnp.bfloat16)
    skip_term = term(normed_low, grad_hidden_low)
    grad_normed = back_product(grad_hidden_low, skip_full)
    grad_joined, gain_cat_grad, bias_cat_grad = joined_pull(grad_normed)

    if links.ring:
        links.sent = []
        down_blocks, down_own = reduce_start_halved(links, *down_terms)
        up_blocks, up_own = reduce_start_halved(links, *up_terms)
        moved = run_steps(
            links,
            {
                "down": reduce_ring(links, down_blocks),
                "up": reduce_ring(links, up_blocks),
                "small": reduce_ring(links, reduce_start(links, small_term)),
                "in": reduce_ring(links, reduce_start(links, in_term)),
                "skip": reduce_ring(links, reduce_start(links, skip_term)),
            },
            ["down", "down", "up", "down", "up", "down", "up", "up"]
            + ["small"] * 4
            + ["in"] * 4
            + ["skip"] * 4,
        )
        down_first, down_second = reduce_finish_halved(
            links, down_terms[0], down_own, moved["down"]
        )
        up_first, up_second = reduce_finish_halved(links, up_terms[0], up_own, moved["up"])
        small_sum = reduce_finish(links, small_term, moved["small"])
        in_sum = reduce_finish(links, in_term, moved["in"])
        skip_sum = reduce_finish(links, skip_term, moved["skip"])
    else:

        def reduced(stack):
            part = lax.psum_scatter(
                stack.astype(jnp.float32), "shard", scatter_dimension=0, tiled=True
            )[0]
            return part.astype(jnp.bfloat16)

        def ordered(pair):
            first = jnp.where(links.side == 0, pair[0], pair[1])
            second = jnp.where(links.side == 0, pair[1], pair[0])
            return [
                lax.psum(reduced(part), "rep").astype(jnp.float32) for part in (first, second)
            ]

        down_first, down_second = ordered(down_terms)
        up_first, up_second = ordered(up_terms)
        small_sum, in_sum, skip_sum = (
            lax.psum(reduced(stack), "rep").astype(jnp.float32)
            for stack in (small_term, in_term, skip_term)
        )
    down_sum = jnp.concatenate([down_first, down_second], 0)
    up_sum = jnp.stack(
        [up_first.reshape(own_rows, n, slab), up_second.reshape(own_rows, n, slab)], 2
    ).reshape(own_rows, hidden_units)
    small_sums = [small_sum[low:high] for low, high in small_parts]
    keyval_sum = jnp.concatenate(small_sums[3:], 1)

    all_shifts = lax.all_gather(shift_grads, ("rep", "shard"), axis=0)
    all_shifts = jnp.sum(all_shifts.reshape(rep_count, n * batches, D), 0)
    shift_sum = lax.dot_general(
        silu_cols.astype(jnp.float32),
        all_shifts,
        (((0,), (0,)), ((), ())),
        precision=lax.Precision.HIGHEST,
    )

    up_bias_sum = jnp.stack(
        [
            jnp.where(links.side == 0, grad_up_sums[0], grad_up_sums[1]).reshape(n, slab),
            jnp.where(links.side == 0, grad_up_sums[1], grad_up_sums[0]).reshape(n, slab),
        ],
        1,
    )
    vector_terms = [
        gain_cat_grad,
        gain_first,
        gain_mid,
        gain_last,
        bias_cat_grad,
        jnp.sum(grad_hidden, 0),
        bias_first,
        jnp.sum(shift_grads, 0),
        jnp.sum(grad_proj, 0),
        jnp.sum(grad_two, 0),
        bias_mid,
        jnp.sum(grad_cq_raw, 0),
        jnp.sum(grad_tk_raw, 0),
        jnp.sum(grad_tv_raw, 0),
        jnp.sum(grad_three, 0),
        bias_last,
        jnp.sum(grad_out, 0),
        up_bias_sum.reshape(-1),
        self_qgain_grad,
        self_kgain_grad,
        cross_gain_grad,
        text_gain_grad,
        self_qbias_grad,
        self_kbias_grad,
        cross_bias_grad,
    ]
    summed = lax.psum(jnp.concatenate(vector_terms), ("rep", "shard"))
    line_count = norm_gains.shape[0] + bias_rows.shape[0]
    lines = summed[: line_count * D].reshape(line_count, D)
    own_lines = lax.dynamic_slice_in_dim(lines, links.shard * own_rows, own_rows, 1)
    rest = summed[line_count * D :]
    own_bias = lax.dynamic_slice_in_dim(rest[:hidden_units], links.shard * 2 * slab, 2 * slab, 0)
    heads = rest[hidden_units:].reshape(-1, HD)
    return (
        activations,
        grad_joined[:, :D].reshape(latents.shape),
        grad_joined[:, D:].reshape(latents.shape),
        text_grad.reshape(text_states.shape),
        skip_sum,
        shift_sum,
        in_sum,
        small_sums[0],
        small_sums[1],
        keyval_sum,
        small_sums[2],
        up_sum,
        down_sum,
        own_lines[: norm_gains.shape[0]],
        own_lines[norm_gains.shape[0] :],
        own_bias,
        heads[: head_gains.shape[0]],
        heads[head_gains.shape[0] :],
    )


def solution(mesh):
    in_specs = (
        P(None, "shard", "rep", None),
        P(None, "shard", "rep", None),
        P(None, "shard", None, None),
        P(None, "shard", None),
        P(None, "shard", "rep", None),
        P("shard", None),
        P("shard", None),
        P("shard", None),
        P("shard", None),
        P("shard", None),
        P("shard", None),
        P("shard", None),
        P("shard", None),
        P("shard", None),
        P(None, "shard"),
        P(None, "shard"),
        P("shard"),
        P(),
        P(),
    )
    out_specs = (
        P(None, "shard", "rep", None),
        P(None, "shard", "rep", None),
        P(None, "shard", "rep", None),
        P(None, "shard", None, None),
        P("shard", None),
        P("shard", None),
        P("shard", None),
        P("shard", None),
        P("shard", None),
        P("shard", None),
        P("shard", None),
        P("shard", None),
        P("shard", None),
        P(None, "shard"),
        P(None, "shard"),
        P("shard"),
        P(),
        P(),
    )
    block = partial(shards, mesh.shape["shard"], mesh.shape["rep"])
    return jax.shard_map(block, mesh=mesh, in_specs=in_specs, out_specs=out_specs, check_vma=False)
```
